32 devices in a mesh: row: 4 (over y, x), col: 8 (over z, core).
Axes of the slice: x: 2, y: 2, z: 4, core: 2. Of those that a mesh axis runs over, the one named last changes fastest.
Arguments:
- old_residual: float32 [1024, 16384], P(('row', 'col')), may hold values from -6 to 6
- group_map: int32 [32, 4], replicated, may hold values from 0 to 127, as said below
- q_factor: float32 [16384, 32], P('col', 'row'), may hold values from -0.046875 to 0.046875
Outputs:
- relaid: float32 [1024, 16384], P('row', 'col')
- projection: float32 [32, 1024], P(None, ('row', 'col'))
- row_norms: float32 [1024], P(('row', 'col'))
The draws below stay inside these ranges and needn't reach their ends.
Inputs may be any that keep to these rules, and one draw needn't show every extreme that they name: `group_map`: all entries together are each group id 0 to 127 once; row d (old device d) holds exactly one id of each range k * 32 to (k + 1) * 32 - 1, in any slot order.
All inputs are finite; a program needn't handle non-finite values.
Results may differ from the reference program's by a relative error of at most 0.00007.
Values sent between devices are 32-bit elements; how exact they have to be, the bound alone decides.
A program may use at most 64 MiB of HBM per device.

```python
import jax
import jax.numpy as jnp
from jax import lax

D = 16384
RANK = 32
CH = 8
ROWS = 1024
N_ROW = 4
DEVICES = 32


def draw_group_map(key, part):
    first_key = jax.random.fold_in(key, 11)
    second_key = jax.random.fold_in(key, 23)
    block_keys = jax.random.split(first_key, N_ROW)
    permuted = jax.vmap(lambda single: jax.random.permutation(single, DEVICES))(block_keys)
    group_ids = (permuted + jnp.arange(N_ROW, dtype=jnp.int32)[:, None] * DEVICES).T
    slot_keys = jax.random.split(second_key, DEVICES)
    slot_order = jax.vmap(lambda single: jax.random.permutation(single, N_ROW))(slot_keys)
    return jnp.take_along_axis(group_ids, slot_order, axis=1).astype(jnp.int32)


def shard_levels(key, shape, pieces, low, high):
    gain = 1.0
    for position, parts in pieces:
        steps = jax.random.uniform(jax.random.fold_in(jax.random.fold_in(key, 6), position), (parts,), jnp.float32, low / len(pieces), high / len(pieces))
        gain = gain * jnp.repeat(jnp.exp(steps), shape[position] // parts).reshape((-1,) + (1,) * (len(shape) - 1 - position))
    return gain


def normal_values(key, shape, deviation, bound, pieces=(), kind=jnp.bfloat16):
    array = deviation * jax.random.normal(key, shape, jnp.float32)
    if pieces:
        array = array * shard_levels(key, shape, pieces, -0.22, 0.18)
    return jnp.clip(array, -bound, bound).astype(kind)


def setup_inputs(seed: int = 0) -> dict:
    streams_of = jax.random.split(jax.random.key(seed), 4)
    return {
        "old_residual": normal_values(streams_of[0], (ROWS, D), 1.0, 6.0, ((0, 32),), jnp.float32),
        "group_map": draw_group_map(jax.random.fold_in(streams_of[3], 71), 0),
        "q_factor": normal_values(streams_of[2], (D, RANK), D ** -0.5, 0.046875, ((0, 8), (1, 4)), jnp.float32),
    }


epsilon = 1e-06

def reference(old_residual, group_map, q_factor):
    group_ids = group_map.reshape(-1).astype(jnp.int32)
    ordering = jnp.argsort(group_ids).astype(jnp.int32)
    groups = old_residual.reshape(DEVICES * N_ROW, CH, D)
    relaid = jnp.take(groups, ordering, axis=0).reshape(ROWS, D)
    product = jnp.dot(relaid, q_factor, precision=lax.Precision.HIGHEST, preferred_element_type=jnp.float32)
    row_norms = jnp.sqrt(lax.optimization_barrier(jnp.mean(relaid * relaid, axis=1)) + epsilon)
    return (relaid, product.T, row_norms)
```

```python
import functools

import jax
import jax.numpy as jnp
from jax import lax
from jax.experimental import pallas as pl
from jax.experimental.pallas import tpu as pltpu
from jax.sharding import PartitionSpec as P

epsilon = 1e-06
MESH = pl.DeviceIdType.MESH


def flip(x, bits):
    b = 1
    while b <= bits:
        if bits & b:
            x = x + b * (1 - 2 * lax.rem(lax.div(x, b), 2))
        b *= 2
    return x


def kernel(
    rows, cols, map_ref, old_ref, q_ref,
    out_ref, proj_ref, sums_ref,
    old, picked, recv, qbuf, qwide, part, squares, tail_out, tail_in,
    ids, inverse,
    in_sem, own_sem, send_sem, recv_sem, q_send, q_recv, q_own, t_send, t_recv,
):
    total = rows * cols
    my_row, my_col = lax.axis_index("row"), lax.axis_index("col")
    me = my_row * cols + my_col
    group = old.shape[1]
    width = recv.shape[2]
    rank_part = qbuf.shape[1]
    rank = rows * rank_part
    lanes = rows * rank

    fetch = pltpu.make_async_copy(old_ref, old, in_sem)
    fetch.start()
    q_fetch = pltpu.make_async_copy(q_ref, qbuf.at[my_row], q_own)
    q_fetch.start()

    barrier = pltpu.get_barrier_semaphore()
    for u in range(rows):
        for v in range(cols):
            if u or v:
                pl.semaphore_signal(
                    barrier, inc=1, device_id=(flip(my_row, u), flip(my_col, v)), device_id_type=MESH
                )

    fetch.wait()
    for k in range(rows):
        slot = 0
        for j in range(rows):
            slot = jnp.where(lax.div(map_ref[me, j], total) == k, j, slot)
        picked[k] = old[slot]
    q_fetch.wait()
    pl.semaphore_wait(barrier, total - 1)

    def piece(r, c):
        return picked.at[r, :, pl.ds(pl.multiple_of(c * width, width), width)]

    def move(u, v):
        r, c = flip(my_row, u), flip(my_col, v)
        return pltpu.make_async_remote_copy(
            src_ref=piece(r, c),
            dst_ref=recv.at[me],
            send_sem=send_sem.at[r * cols + c],
            recv_sem=recv_sem.at[me],
            device_id=(r, c),
            device_id_type=MESH,
        )

    def arrival(u, v):
        r, c = flip(my_row, u), flip(my_col, v)
        source = r * cols + c
        return pltpu.make_async_remote_copy(
            src_ref=piece(r, c),
            dst_ref=recv.at[source],
            send_sem=send_sem.at[source],
            recv_sem=recv_sem.at[source],
            device_id=(r, c),
            device_id_type=MESH,
        )

    def q_move(u, slot):
        return pltpu.make_async_remote_copy(
            src_ref=qbuf.at[my_row],
            dst_ref=qbuf.at[slot],
            send_sem=q_send.at[flip(my_row, u)],
            recv_sem=q_recv.at[slot],
            device_id=(flip(my_row, u), my_col),
            device_id_type=MESH,
        )

    far = [v for v in range(cols - 1, -1, -1) if v >= cols // 2]
    near = [v for v in range(cols - 1, -1, -1) if v < cols // 2]
    for v in far:
        for u in range(rows):
            move(u, v).start()
    for u in range(1, rows):
        q_move(u, my_row).start()
    for v in near:
        for u in range(rows):
            if u or v:
                move(u, v).start()
    own = pltpu.make_async_copy(piece(my_row, my_col), recv.at[me], own_sem)
    own.start()

    def read_ids(d, _):
        found = 0
        for j in range(rows):
            value = map_ref[d, j]
            found = jnp.where(lax.div(value, total) == my_row, value - my_row * total, found)
        ids[d] = found
        return 0

    lax.fori_loop(0, total, read_ids, 0)

    def invert(g, _):
        found = 0
        for d in range(total):
            found = jnp.where(ids[d] == g, d, found)
        inverse[g] = found
        return 0

    lax.fori_loop(0, total, invert, 0)

    for u in range(1, rows):
        q_move(u, flip(my_row, u)).wait_recv()
    for m in range(rows):
        for k in range(rows):
            qwide[pl.ds(m * rank + k * rank_part, rank_part), :] = qbuf[k]

    own.wait()
    for v in near[::-1] + far:
        for u in range(rows):
            if u or v:
                arrival(u, v).wait_recv()
        sources = [flip(my_row, u) * cols + flip(my_col, v) for u in range(rows)]
        block = jnp.concatenate([recv[s] for s in sources], axis=0)
        product = lax.dot_general(
            block,
            qwide[...],
            (((1,), (1,)), ((), ())),
            precision=lax.Precision.HIGHEST,
            preferred_element_type=jnp.float32,
        )
        row_sums = jnp.sum(block * block, axis=1, keepdims=True)
        for u in range(rows):
            part[sources[u]] = product[u * group:(u + 1) * group]
            squares[sources[u]] = jnp.broadcast_to(row_sums[u * group:(u + 1) * group], (group, 128))

    p_lane = lax.broadcasted_iota(jnp.int32, (group, lanes), 1)
    s_lane = lax.broadcasted_iota(jnp.int32, (group, 128), 1)
    for c in range(cols):
        p_tile = jnp.zeros((group, lanes), jnp.float32)
        s_tile = jnp.zeros((group, 128), jnp.float32)
        for m in range(rows):
            source = inverse[c * rows + m]
            p_tile = jnp.where(lax.div(p_lane, rank) == m, part[source], p_tile)
            s_tile = jnp.where(s_lane == m, squares[source], s_tile)
        tail_out[c, :, pl.ds(0, lanes)] = p_tile
        tail_out[c, :, pl.ds(lanes, 128)] = s_tile

    def tail(v, slot):
        c = flip(my_col, v)
        return pltpu.make_async_remote_copy(
            src_ref=tail_out.at[c],
            dst_ref=tail_in.at[slot],
            send_sem=t_send.at[c],
            recv_sem=t_recv.at[slot],
            device_id=(my_row, c),
            device_id_type=MESH,
        )

    for v in range(cols - 1, 0, -1):
        tail(v, my_col).start()

    for g in range(total):
        out_ref[g] = recv[inverse[g]]

    result = tail_out[my_col]
    for v in range(1, cols):
        c = flip(my_col, v)
        tail(v, c).wait_recv()
        result = result + tail_in[c]
    turned = result[:, :lanes].T
    for m in range(rows):
        proj_ref[:, pl.ds(m * group, group)] = turned[m * rank:(m + 1) * rank, :]
    sums_ref[...] = jnp.sqrt(result[:, lanes:] / (width * cols) + epsilon)

    for u in range(rows):
        for v in range(cols):
            if u or v:
                move(u, v).wait_send()
    for u in range(1, rows):
        q_move(u, my_row).wait_send()
    for v in range(1, cols):
        tail(v, my_col).wait_send()


def on_device(rows, cols, old_residual, group_map, q_factor):
    total = rows * cols
    height, full = old_residual.shape
    group = height // rows
    width = full // cols
    depth, rank_part = q_factor.shape
    rank = rank_part * rows
    lanes = rows * rank
    f32 = jnp.float32
    hbm = pl.BlockSpec(memory_space=pl.ANY)
    vmem = pl.BlockSpec(memory_space=pltpu.VMEM)
    dma = pltpu.SemaphoreType.DMA
    relaid, projection, norms = pl.pallas_call(
        functools.partial(kernel, rows, cols),
        out_shape=[
            jax.ShapeDtypeStruct((total, group, width), f32),
            jax.ShapeDtypeStruct((rank, rows * group), f32),
            jax.ShapeDtypeStruct((group, 128), f32),
        ],
        in_specs=[pl.BlockSpec(memory_space=pltpu.SMEM), hbm, hbm],
        out_specs=[vmem, vmem, vmem],
        scratch_shapes=[
            pltpu.VMEM((rows, group, full), f32),
            pltpu.VMEM((rows, group, full), f32),
            pltpu.VMEM((total, group, width), f32),
            pltpu.VMEM((rows, rank_part, depth), f32),
            pltpu.VMEM((lanes, depth), f32),
            pltpu.VMEM((total, group, lanes), f32),
            pltpu.VMEM((total, group, 128), f32),
            pltpu.VMEM((cols, group, lanes + 128), f32),
            pltpu.VMEM((cols, group, lanes + 128), f32),
            pltpu.SMEM((total,), jnp.int32),
            pltpu.SMEM((total,), jnp.int32),
            dma, dma,
            dma((total,)), dma((total,)),
            dma((rows,)), dma((rows,)), dma,
            dma((cols,)), dma((cols,)),
        ],
        compiler_params=pltpu.CompilerParams(
            collective_id=0, has_side_effects=True, vmem_limit_bytes=50 * 1024 * 1024
        ),
    )(group_map, old_residual.reshape(rows, group, full), q_factor.T)
    return (
        relaid.reshape(total * group, width),
        projection,
        norms[:, :rows].T.reshape(rows * group),
    )


def solution(mesh):
    rows, cols = mesh.shape["row"], mesh.shape["col"]
    placed = (P(("row", "col"), None), P(), P("col", "row"))
    return jax.shard_map(
        functools.partial(on_device, rows, cols),
        mesh=mesh,
        in_specs=placed,
        out_specs=(P("row", "col"), P(None, ("row", "col")), P(("row", "col"))),
        check_vma=False,
    )
```

```python
import functools

import jax
import jax.numpy as jnp
from jax import lax
from jax.experimental import pallas as pl
from jax.experimental.pallas import tpu as pltpu
from jax.sharding import PartitionSpec as P

epsilon = 1e-06
MESH = pl.DeviceIdType.MESH


def flip(x, bits):
    b = 1
    while b <= bits:
        if bits & b:
            x = x + b * (1 - 2 * lax.rem(lax.div(x, b), 2))
        b *= 2
    return x


def kernel(
    rows, cols, map_ref, old_ref, q_ref,
    recv, proj_ref, norm_ref,
    old, picked, qbuf, part, squares, tail_out, tail_in,
    ids, inverse,
    in_sems, own_sem, send_sem, recv_sem, q_send, q_recv, q_own, t_send, t_recv,
):
    total = rows * cols
    my_row, my_col = lax.axis_index("row"), lax.axis_index("col")
    me = my_row * cols + my_col
    group = recv.shape[1]
    width = recv.shape[2]
    rank_part = qbuf.shape[1]
    rank = rows * rank_part
    lanes = rows * rank

    barrier = pltpu.get_barrier_semaphore()
    for u in range(rows):
        for v in range(cols):
            if u or v:
                pl.semaphore_signal(
                    barrier, inc=1, device_id=(flip(my_row, u), flip(my_col, v)), device_id_type=MESH
                )

    order = [v for v in range(cols - 1, -1, -1)]
    far, near = order[:cols // 2], order[cols // 2:]

    def fetch(v):
        start = pl.multiple_of(flip(my_col, v) * width, width)
        return pltpu.make_async_copy(old_ref.at[:, :, pl.ds(start, width)], old[v], in_sems.at[v])

    for v in order:
        fetch(v).start()
    q_fetch = pltpu.make_async_copy(q_ref, qbuf.at[my_row], q_own)
    q_fetch.start()

    def slot_of(r):
        slot = 0
        for j in range(rows):
            slot = jnp.where(lax.div(map_ref[j, me], total) == r, j, slot)
        return slot

    partners = [flip(my_row, u) for u in range(rows)]
    slots = [slot_of(r) for r in partners]

    def pick(v):
        fetch(v).wait()
        for u in range(rows):
            picked[v, u] = old[v][slots[u]]

    def move(u, v):
        r, c = flip(my_row, u), flip(my_col, v)
        return pltpu.make_async_remote_copy(
            src_ref=picked.at[v, u],
            dst_ref=recv.at[me],
            send_sem=send_sem.at[r * cols + c],
            recv_sem=recv_sem.at[me],
            device_id=(r, c),
            device_id_type=MESH,
        )

    def arrival(u, v):
        r, c = flip(my_row, u), flip(my_col, v)
        source = r * cols + c
        return pltpu.make_async_remote_copy(
            src_ref=picked.at[v, u],
            dst_ref=recv.at[source],
            send_sem=send_sem.at[source],
            recv_sem=recv_sem.at[source],
            device_id=(r, c),
            device_id_type=MESH,
        )

    def q_move(u, slot):
        return pltpu.make_async_remote_copy(
            src_ref=qbuf.at[my_row],
            dst_ref=qbuf.at[slot],
            send_sem=q_send.at[flip(my_row, u)],
            recv_sem=q_recv.at[slot],
            device_id=(flip(my_row, u), my_col),
            device_id_type=MESH,
        )

    pick(far[0])
    pl.semaphore_wait(barrier, total - 1)
    for v in far:
        if v != far[0]:
            pick(v)
        for u in range(rows):
            move(u, v).start()
    q_fetch.wait()
    for u in range(1, rows):
        q_move(u, my_row).start()
    for v in near:
        pick(v)
        for u in range(rows):
            if u or v:
                move(u, v).start()
    own = pltpu.make_async_copy(picked.at[0, 0], recv.at[me], own_sem)
    own.start()

    def read_ids(d, _):
        found = 0
        for j in range(rows):
            value = map_ref[j, d]
            found = jnp.where(lax.div(value, total) == my_row, value - my_row * total, found)
        ids[d] = found
        return 0

    lax.fori_loop(0, total, read_ids, 0)

    def invert(g, _):
        found = 0
        for d in range(total):
            found = jnp.where(ids[d] == g, d, found)
        inverse[g] = found
        return 0

    lax.fori_loop(0, total, invert, 0)

    for u in range(1, rows):
        q_move(u, flip(my_row, u)).wait_recv()
    factor = qbuf[...].reshape(rank, width)
    own.wait()
    for v in near[::-1] + far:
        for u in range(rows):
            if u or v:
                arrival(u, v).wait_recv()
        sources = [flip(my_row, u) * cols + flip(my_col, v) for u in range(rows)]
        block = jnp.concatenate([recv[s] for s in sources], axis=0)
        product = lax.dot_general(
            block,
            factor,
            (((1,), (1,)), ((), ())),
            precision=lax.Precision.HIGHEST,
            preferred_element_type=jnp.float32,
        )
        row_sums = jnp.sum(block * block, axis=1, keepdims=True)
        for u in range(rows):
            own_rows = product[u * group:(u + 1) * group]
            part[sources[u]] = jnp.concatenate([own_rows] * rows, axis=1)
            squares[sources[u]] = jnp.broadcast_to(row_sums[u * group:(u + 1) * group], (group, 128))

    p_lane = lax.broadcasted_iota(jnp.int32, (group, lanes), 1)
    s_lane = lax.broadcasted_iota(jnp.int32, (group, 128), 1)
    for c in range(cols):
        p_tile = jnp.zeros((group, lanes), jnp.float32)
        s_tile = jnp.zeros((group, 128), jnp.float32)
        for m in range(rows):
            source = inverse[c * rows + m]
            p_tile = jnp.where(lax.div(p_lane, rank) == m, part[source], p_tile)
            s_tile = jnp.where(s_lane == m, squares[source], s_tile)
        tail_out[c, :, pl.ds(0, lanes)] = p_tile
        tail_out[c, :, pl.ds(lanes, 128)] = s_tile

    def tail(v, slot):
        c = flip(my_col, v)
        return pltpu.make_async_remote_copy(
            src_ref=tail_out.at[c],
            dst_ref=tail_in.at[slot],
            send_sem=t_send.at[c],
            recv_sem=t_recv.at[slot],
            device_id=(my_row, c),
            device_id_type=MESH,
        )

    for v in range(cols - 1, 0, -1):
        tail(v, my_col).start()

    result = tail_out[my_col]
    for v in range(1, cols):
        c = flip(my_col, v)
        tail(v, c).wait_recv()
        result = result + tail_in[c]
    turned = result[:, :lanes].T
    for m in range(rows):
        proj_ref[:, pl.ds(m * group, group)] = turned[m * rank:(m + 1) * rank, :]
    norms = jnp.sqrt(result[:, lanes:] / (width * cols) + epsilon).T
    for m in range(rows):
        norm_ref[:, pl.ds(m * group, group)] = norms[m:m + 1, :]

    for u in range(rows):
        for v in range(cols):
            if u or v:
                move(u, v).wait_send()
    for u in range(1, rows):
        q_move(u, my_row).wait_send()
    for v in range(1, cols):
        tail(v, my_col).wait_send()


def place(rows, cols, map_ref, recv, proj_in, norm_in, out_ref, proj_ref, norm_ref, sems, small_sems):
    total = rows * cols
    my_row = lax.axis_index("row")
    smalls = [
        pltpu.make_async_copy(proj_in, proj_ref, small_sems.at[0]),
        pltpu.make_async_copy(norm_in, norm_ref, small_sems.at[1]),
    ]
    for d in range(total):
        where = 0
        for j in range(rows):
            value = map_ref[j, d]
            where = jnp.where(lax.div(value, total) == my_row, value - my_row * total, where)
        pltpu.make_async_copy(recv.at[d], out_ref.at[where], sems.at[d]).start()
    for small in smalls:
        small.start()
    for d in range(total):
        pltpu.make_async_copy(recv.at[d], out_ref.at[d], sems.at[d]).wait()
    for small in smalls:
        small.wait()


def on_device(rows, cols, old_residual, group_map, q_factor):
    total = rows * cols
    height, full = old_residual.shape
    group = height // rows
    width = full // cols
    depth, rank_part = q_factor.shape
    rank = rank_part * rows
    lanes = rows * rank
    f32 = jnp.float32
    hbm = pl.BlockSpec(memory_space=pltpu.HBM)
    vmem = pl.BlockSpec(memory_space=pltpu.VMEM)
    dma = pltpu.SemaphoreType.DMA
    map_turned = group_map.T
    shapes = [
        jax.ShapeDtypeStruct((total, group, width), f32),
        jax.ShapeDtypeStruct((rank, rows * group), f32),
        jax.ShapeDtypeStruct((1, rows * group), f32),
    ]
    smem = pl.BlockSpec(memory_space=pltpu.SMEM)
    arrived = pl.pallas_call(
        functools.partial(kernel, rows, cols),
        out_shape=shapes,
        in_specs=[smem, hbm, hbm],
        out_specs=[vmem, vmem, vmem],
        scratch_shapes=[
            [pltpu.VMEM((rows, group, width), f32)] * cols,
            pltpu.VMEM((cols, rows, group, width), f32),
            pltpu.VMEM((rows, rank_part, depth), f32),
            pltpu.VMEM((total, group, lanes), f32),
            pltpu.VMEM((total, group, 128), f32),
            pltpu.VMEM((cols, group, lanes + 128), f32),
            pltpu.VMEM((cols, group, lanes + 128), f32),
            pltpu.SMEM((total,), jnp.int32),
            pltpu.SMEM((total,), jnp.int32),
            dma((cols,)), dma,
            dma((total,)), dma((total,)),
            dma((rows,)), dma((rows,)), dma,
            dma((cols,)), dma((cols,)),
        ],
        compiler_params=pltpu.CompilerParams(
            collective_id=0, has_side_effects=True, vmem_limit_bytes=50 * 1024 * 1024
        ),
    )(map_turned, old_residual.reshape(rows, group, full), q_factor.T)
    relaid, projection, norms = pl.pallas_call(
        functools.partial(place, rows, cols),
        out_shape=shapes,
        in_specs=[smem, vmem, vmem, vmem],
        out_specs=[hbm, hbm, hbm],
        scratch_shapes=[dma((total,)), dma((2,))],
        compiler_params=pltpu.CompilerParams(vmem_limit_bytes=8 * total * group * width),
    )(map_turned, *arrived)
    return relaid.reshape(total * group, width), projection, norms.reshape(rows * group)


def solution(mesh):
    rows, cols = mesh.shape["row"], mesh.shape["col"]
    placed = (P(("row", "col"), None), P(), P("col", "row"))
    return jax.shard_map(
        functools.partial(on_device, rows, cols),
        mesh=mesh,
        in_specs=placed,
        out_specs=(P("row", "col"), P(None, ("row", "col")), P(("row", "col"))),
        check_vma=False,
    )
```

```python
import functools

import jax
import jax.numpy as jnp
from jax import lax
from jax.experimental import pallas as pl
from jax.experimental.pallas import tpu as pltpu
from jax.sharding import PartitionSpec as P

epsilon = 1e-06
MESH = pl.DeviceIdType.MESH


def flip(x, bits):
    b = 1
    while b <= bits:
        if bits & b:
            x = x + b * (1 - 2 * lax.rem(lax.div(x, b), 2))
        b *= 2
    return x


def kernel(
    rows, cols, map_ref, old_ref, q_ref,
    recv, proj_ref, norm_ref,
    old, picked, qbuf, part, squares, tail_out, tail_in,
    ids, inverse,
    in_sems, own_sem, send_sem, recv_sem, q_send, q_recv, q_own, t_send, t_recv,
):
    total = rows * cols
    my_row, my_col = lax.axis_index("row"), lax.axis_index("col")
    me = my_row * cols + my_col
    group = recv.shape[1]
    width = recv.shape[2]
    rank_part = qbuf.shape[1]
    rank = rows * rank_part
    lanes = rows * rank

    barrier = pltpu.get_barrier_semaphore()
    for u in range(rows):
        for v in range(cols):
            if u or v:
                pl.semaphore_signal(
                    barrier, inc=1, device_id=(flip(my_row, u), flip(my_col, v)), device_id_type=MESH
                )

    order = [v for v in range(cols - 1, -1, -1)]
    far, near = order[:cols // 2], order[cols // 2:]

    def fetch(v):
        start = pl.multiple_of(flip(my_col, v) * width, width)
        return pltpu.make_async_copy(old_ref.at[:, :, pl.ds(start, width)], old[v], in_sems.at[v])

    for v in order:
        fetch(v).start()
    q_fetch = pltpu.make_async_copy(q_ref, qbuf.at[my_row], q_own)
    q_fetch.start()

    def slot_of(r):
        slot = 0
        for j in range(rows):
            slot = jnp.where(lax.div(map_ref[j, me], total) == r, j, slot)
        return slot

    partners = [flip(my_row, u) for u in range(rows)]
    slots = [slot_of(r) for r in partners]

    def pick(v):
        fetch(v).wait()
        for u in range(rows):
            picked[v, u] = old[v][slots[u]]

    def move(u, v):
        r, c = flip(my_row, u), flip(my_col, v)
        return pltpu.make_async_remote_copy(
            src_ref=picked.at[v, u],
            dst_ref=recv.at[me],
            send_sem=send_sem.at[r * cols + c],
            recv_sem=recv_sem.at[me],
            device_id=(r, c),
            device_id_type=MESH,
        )

    def arrival(u, v):
        r, c = flip(my_row, u), flip(my_col, v)
        source = r * cols + c
        return pltpu.make_async_remote_copy(
            src_ref=picked.at[v, u],
            dst_ref=recv.at[source],
            send_sem=send_sem.at[source],
            recv_sem=recv_sem.at[source],
            device_id=(r, c),
            device_id_type=MESH,
        )

    def q_move(u, slot):
        return pltpu.make_async_remote_copy(
            src_ref=qbuf.at[my_row],
            dst_ref=qbuf.at[slot],
            send_sem=q_send.at[flip(my_row, u)],
            recv_sem=q_recv.at[slot],
            device_id=(flip(my_row, u), my_col),
            device_id_type=MESH,
        )

    pick(far[0])
    pl.semaphore_wait(barrier, total - 1)
    for v in far:
        if v != far[0]:
            pick(v)
        for u in range(rows):
            move(u, v).start()
    q_fetch.wait()
    for u in range(1, rows):
        q_move(u, my_row).start()
    for v in near:
        pick(v)
        for u in range(rows):
            if u or v:
                move(u, v).start()
    own = pltpu.make_async_copy(picked.at[0, 0], recv.at[me], own_sem)
    own.start()

    def read_ids(d, _):
        found = 0
        for j in range(rows):
            value = map_ref[j, d]
            found = jnp.where(lax.div(value, total) == my_row, value - my_row * total, found)
        ids[d] = found
        return 0

    lax.fori_loop(0, total, read_ids, 0)

    def invert(g, _):
        found = 0
        for d in range(total):
            found = jnp.where(ids[d] == g, d, found)
        inverse[g] = found
        return 0

    lax.fori_loop(0, total, invert, 0)

    for u in range(1, rows):
        q_move(u, flip(my_row, u)).wait_recv()
    factor = qbuf[...].reshape(rank, width)
    own.wait()
    for v in near[::-1] + far:
        for u in range(rows):
            if u or v:
                arrival(u, v).wait_recv()
        sources = [flip(my_row, u) * cols + flip(my_col, v) for u in range(rows)]
        block = jnp.concatenate([recv[s] for s in sources], axis=0)
        product = lax.dot_general(
            block,
            factor,
            (((1,), (1,)), ((), ())),
            precision=lax.Precision.HIGHEST,
            preferred_element_type=jnp.float32,
        )
        row_sums = jnp.sum(block * block, axis=1, keepdims=True)
        for u in range(rows):
            own_rows = product[u * group:(u + 1) * group]
            part[sources[u]] = jnp.concatenate([own_rows] * rows, axis=1)
            squares[sources[u]] = jnp.broadcast_to(row_sums[u * group:(u + 1) * group], (group, lanes))

    p_lane = lax.broadcasted_iota(jnp.int32, (group, lanes), 1)
    s_lane = lax.broadcasted_iota(jnp.int32, (group, lanes), 1)
    s_row = lax.broadcasted_iota(jnp.int32, (group, lanes), 0)
    for c in range(cols):
        p_tile = jnp.zeros((group, lanes), jnp.float32)
        s_tile = jnp.zeros((group, lanes), jnp.float32)
        for m in range(rows):
            source = inverse[c * rows + m]
            p_tile = jnp.where(lax.div(p_lane, rank) == m, part[source], p_tile)
            s_tile = jnp.where(s_lane == m * group + s_row, squares[source], s_tile)
        tail_out[c, pl.ds(0, group), :] = p_tile
        tail_out[c, pl.ds(group, 1), :] = jnp.sum(s_tile, axis=0, keepdims=True)

    def tail(v, slot):
        c = flip(my_col, v)
        return pltpu.make_async_remote_copy(
            src_ref=tail_out.at[c],
            dst_ref=tail_in.at[slot],
            send_sem=t_send.at[c],
            recv_sem=t_recv.at[slot],
            device_id=(my_row, c),
            device_id_type=MESH,
        )

    for v in range(cols - 1, 0, -1):
        tail(v, my_col).start()

    result = tail_out[my_col]
    for v in range(1, cols):
        c = flip(my_col, v)
        tail(v, c).wait_recv()
        result = result + tail_in[c]
    turned = result[:group].T
    for m in range(rows):
        proj_ref[:, pl.ds(m * group, group)] = turned[m * rank:(m + 1) * rank, :]
    norm_ref[...] = jnp.sqrt(result[group:, :rows * group] / (width * cols) + epsilon)

    for u in range(rows):
        for v in range(cols):
            if u or v:
                move(u, v).wait_send()
    for u in range(1, rows):
        q_move(u, my_row).wait_send()
    for v in range(1, cols):
        tail(v, my_col).wait_send()


def place(rows, cols, map_ref, recv, proj_in, norm_in, out_ref, proj_ref, norm_ref, sems, small_sems):
    total = rows * cols
    my_row = lax.axis_index("row")
    smalls = [
        pltpu.make_async_copy(proj_in, proj_ref, small_sems.at[0]),
        pltpu.make_async_copy(norm_in, norm_ref, small_sems.at[1]),
    ]
    for d in range(total):
        where = 0
        for j in range(rows):
            value = map_ref[j, d]
            where = jnp.where(lax.div(value, total) == my_row, value - my_row * total, where)
        pltpu.make_async_copy(recv.at[d], out_ref.at[where], sems.at[d]).start()
    for small in smalls:
        small.start()
    for d in range(total):
        pltpu.make_async_copy(recv.at[d], out_ref.at[d], sems.at[d]).wait()
    for small in smalls:
        small.wait()


def on_device(rows, cols, old_residual, group_map, q_factor):
    total = rows * cols
    height, full = old_residual.shape
    group = height // rows
    width = full // cols
    depth, rank_part = q_factor.shape
    rank = rank_part * rows
    lanes = rows * rank
    f32 = jnp.float32
    hbm = pl.BlockSpec(memory_space=pltpu.HBM)
    vmem = pl.BlockSpec(memory_space=pltpu.VMEM)
    dma = pltpu.SemaphoreType.DMA
    map_turned = group_map.T
    shapes = [
        jax.ShapeDtypeStruct((total, group, width), f32),
        jax.ShapeDtypeStruct((rank, rows * group), f32),
        jax.ShapeDtypeStruct((1, rows * group), f32),
    ]
    smem = pl.BlockSpec(memory_space=pltpu.SMEM)
    arrived = pl.pallas_call(
        functools.partial(kernel, rows, cols),
        out_shape=shapes,
        in_specs=[smem, hbm, hbm],
        out_specs=[vmem, vmem, vmem],
        scratch_shapes=[
            [pltpu.VMEM((rows, group, width), f32)] * cols,
            pltpu.VMEM((cols, rows, group, width), f32),
            pltpu.VMEM((rows, rank_part, depth), f32),
            pltpu.VMEM((total, group, lanes), f32),
            pltpu.VMEM((total, group, lanes), f32),
            pltpu.VMEM((cols, group + 1, lanes), f32),
            pltpu.VMEM((cols, group + 1, lanes), f32),
            pltpu.SMEM((total,), jnp.int32),
            pltpu.SMEM((total,), jnp.int32),
            dma((cols,)), dma,
            dma((total,)), dma((total,)),
            dma((rows,)), dma((rows,)), dma,
            dma((cols,)), dma((cols,)),
        ],
        compiler_params=pltpu.CompilerParams(
            collective_id=0, has_side_effects=True, vmem_limit_bytes=50 * 1024 * 1024
        ),
    )(
        pltpu.with_memory_space_constraint(map_turned, pltpu.HBM),
        old_residual.reshape(rows, group, full),
        pltpu.with_memory_space_constraint(q_factor.T, pltpu.HBM),
    )
    relaid, projection, norms = pl.pallas_call(
        functools.partial(place, rows, cols),
        out_shape=shapes,
        in_specs=[smem, vmem, vmem, vmem],
        out_specs=[hbm, hbm, hbm],
        scratch_shapes=[dma((total,)), dma((2,))],
        compiler_params=pltpu.CompilerParams(vmem_limit_bytes=8 * total * group * width),
    )(map_turned, *arrived)
    return relaid.reshape(total * group, width), projection, norms.reshape(rows * group)


def solution(mesh):
    rows, cols = mesh.shape["row"], mesh.shape["col"]
    placed = (P(("row", "col"), None), P(), P("col", "row"))
    return jax.shard_map(
        functools.partial(on_device, rows, cols),
        mesh=mesh,
        in_specs=placed,
        out_specs=(P("row", "col"), P(None, ("row", "col")), P(("row", "col"))),
        check_vma=False,
    )
```
